32 devices in a mesh: occ: 4 (over z), vir: 4 (over y, x), ka: 2 (over core).
Axes of the slice: x: 2, y: 2, z: 4, core: 2. Of those that a mesh axis runs over, the one named last changes fastest.
Arguments:
- lambda_amps: bfloat16 [2, 16, 1024, 1024], P(None, 'occ', 'vir', 'ka'), may hold values from -0.25 to 0.25
- screened_ints: bfloat16 [16, 1024, 1024], P(('occ', 'vir'), 'ka'), may hold values from -6 to 6
- half_ints: bfloat16 [16, 1024, 128], P(('occ', 'vir'), 'ka'), may hold values from -0.5 to 0.5
- singles: bfloat16 [128, 1024], P(None, 'vir'), may hold values from -6 to 6
- block_mask: int32 [16, 8, 8], P('occ', 'ka'), may hold values from 0 to 1, as said below
Outputs:
- residual_part: bfloat16 [2, 16, 1024, 1024], P('ka', 'occ', 'vir')
The draws below stay inside these ranges and needn't reach their ends.
Inputs may be any that keep to these rules, and one draw needn't show every extreme that they name: `block_mask`: for each j and each of the 2 equal ranges of e blocks, between 1 and 16 of its 32 blocks are 1; some (j, range) has exactly 16.
All inputs are finite; a program needn't handle non-finite values.
Results may differ from the reference program's by a relative error of at most 0.0058.
Values may be sent and summed in bfloat16 or wider, within the bound.
A program may use at most 128 MiB of HBM per device.

```python
import jax
import jax.numpy as jnp
from jax import lax

O = 128
V = 1024
TILE = 128
CAP = 16
IW = 2
NB = 8
HALVES = 2
HT = 32
J = 16


def draw_block_mask(key, part):
    first_key, second_key, third_key = jax.random.split(key, 3)
    groups = J * HALVES
    base_draw = jax.random.randint(first_key, (groups,), 1, 6)
    counts = jnp.minimum(base_draw * base_draw, CAP)
    forced = jax.random.randint(second_key, (), 0, groups)
    counts = jnp.where(jnp.arange(groups) == forced, CAP, counts)
    scores = jax.random.randint(third_key, (groups, HT), 0, 1 << 20) * HT + jnp.arange(HT)[None, :]
    ordering = jnp.argsort(scores, axis=1, stable=True)
    ranking = jnp.argsort(ordering, axis=1, stable=True)
    live_tiles = (ranking < counts[:, None]).astype(jnp.int32)
    return live_tiles.reshape(J, NB, NB)


def levels(stream_key, shape, cuts, smallest, largest):
    def one(dim, shards_of):
        heights = jax.random.uniform(jax.random.fold_in(jax.random.fold_in(stream_key, 6), dim), (shards_of,), jnp.float32, smallest / len(cuts), largest / len(cuts))
        return jnp.repeat(jnp.exp(heights), shape[dim] // shards_of).reshape((-1,) + (1,) * (len(shape) - dim - 1))

    factor_of = one(*cuts[0])
    for cut in cuts[1:]:
        factor_of = factor_of * one(*cut)
    return factor_of


def gaussian(own_key, shape, deviation, bound, shards=(), dtype=jnp.bfloat16):
    loudness = levels(own_key, shape, shards, -0.22, 0.18) if shards else 1.0
    values = jax.random.normal(own_key, shape, jnp.float32) * deviation * loudness
    return jnp.minimum(jnp.maximum(values, -bound), bound).astype(dtype)


def setup_inputs(seed: int = 0) -> dict:
    key_list = jax.random.split(jax.random.key(seed), 6)
    return {
        "lambda_amps": gaussian(key_list[0], (IW, J, V, V), (V // 2) ** -0.5, 0.25, ((1, 4), (2, 4), (3, 2))),
        "screened_ints": gaussian(key_list[1], (J, V, V), 1.0, 6.0, ((0, 16), (1, 2))),
        "half_ints": gaussian(key_list[2], (J, V, O), O ** -0.5, 0.5, ((0, 16), (1, 2))),
        "singles": gaussian(key_list[3], (O, V), 1.0, 6.0, ((1, 4),)),
        "block_mask": draw_block_mask(jax.random.fold_in(key_list[5], 71), 0),
    }


def reference(lambda_amps, screened_ints, half_ints, singles, block_mask):
    def per_item(item):
        dressed = screened_ints[item].astype(jnp.float32) - jnp.dot(half_ints[item], singles, preferred_element_type=jnp.float32)
        block_gate = jnp.repeat(jnp.repeat(block_mask[item].astype(jnp.float32), TILE, axis=0), TILE, axis=1)
        blocks = (block_gate * dressed).astype(jnp.bfloat16)
        amp_rows = lambda_amps[:, item].reshape(IW * V, V)
        result = jnp.dot(amp_rows, blocks, preferred_element_type=jnp.float32).astype(jnp.bfloat16)
        return result.reshape(IW, V, V)

    stacked = lax.map(per_item, jnp.arange(J).astype(jnp.int32))
    return jnp.transpose(stacked, (1, 0, 2, 3))
```

```python
import functools

import jax
import jax.numpy as jnp
from jax import lax
from jax.experimental import pallas as pl
from jax.experimental.pallas import tpu as pltpu
from jax.sharding import PartitionSpec as P

TILE = 128
CAP = 16
CHUNKS = 4


def peers_of(v, n, grid):
    if grid:
        y, x = v // 2, v % 2
        ids = [v, y * 2 + (1 - x), (1 - y) * 2 + x, (1 - y) * 2 + (1 - x)]
        return ids, ids
    return [(v + k) % n for k in range(n)], [(v + n - k) % n for k in range(n)]


def kernel(n, lam, x, y, t, mask, out, lam_v, x_v, y_v, dressed, dense, own, give, take, res, following,
           in_sem, t_send, t_recv, b_send, b_recv, f_send, p_send, p_recv, o_sem, *bufs):
    t_v, gath = bufs[:n], bufs[n:]
    grid = n == 4
    v, c = lax.axis_index("vir"), lax.axis_index("ka")
    dst, src = peers_of(v, n, grid)
    partner = 1 - c
    half = x_v.shape[0]
    width = t_v[0].shape[1]
    cols = width // TILE
    row_blocks = half // TILE
    col_blocks = x_v.shape[1] // TILE
    blocks = row_blocks * col_blocks
    per = CAP // CHUNKS

    loads = [
        pltpu.make_async_copy(t, t_v[0], in_sem.at[0]),
        pltpu.make_async_copy(y.at[0], y_v, in_sem.at[1]),
        pltpu.make_async_copy(x.at[0], x_v, in_sem.at[2]),
        pltpu.make_async_copy(lam, lam_v, in_sem.at[3]),
    ]
    for load in loads:
        load.start()

    barrier = pltpu.get_barrier_semaphore()
    for k in range(1, n):
        pl.semaphore_signal(barrier, inc=1, device_id={"vir": dst[k]}, device_id_type=pl.DeviceIdType.MESH)
    pl.semaphore_signal(barrier, inc=1, device_id={"ka": partner}, device_id_type=pl.DeviceIdType.MESH)
    loads[0].wait()
    pl.semaphore_wait(barrier, n)

    def remote(source, target, send, recv, where):
        return pltpu.make_async_remote_copy(
            src_ref=source, dst_ref=target, send_sem=send, recv_sem=recv,
            device_id=where, device_id_type=pl.DeviceIdType.MESH)

    t_copies = [None] + [
        remote(t_v[0], t_v[k], t_send.at[k], t_recv.at[k], {"vir": dst[k]}) for k in range(1, n)]
    for copy in t_copies[1:]:
        copy.start()

    following[blocks] = blocks - 1
    later = jnp.int32(blocks - 1)
    for p in reversed(range(blocks)):
        later = jnp.where(mask[v, p // col_blocks, p % col_blocks] != 0, p, later)
        following[p] = later

    loads[1].wait()
    loads[2].wait()

    for k in range(n):
        if k:
            t_copies[k].wait_recv()
        start = src[k] * width
        term = jnp.dot(y_v[...], t_v[k][...], preferred_element_type=jnp.float32)
        part = (x_v[:, pl.ds(pl.multiple_of(start, TILE), width)].astype(jnp.float32) - term).astype(jnp.bfloat16)
        for e in range(row_blocks):
            for b in range(cols):
                dressed[e * col_blocks + src[k] * cols + b] = part[e * TILE:(e + 1) * TILE, b * TILE:(b + 1) * TILE]

    def chunk(ref, q):
        return ref.at[pl.ds(q * per, per)]

    def own_copy(k, q):
        return remote(chunk(gath[0], q), chunk(gath[k], q), b_send.at[k, q], b_recv.at[k, q], {"vir": dst[k]})

    def relay_copy(k, q):
        return remote(chunk(gath[k], q), chunk(gath[3], q), f_send.at[q], b_recv.at[3, q], {"vir": dst[3 - k]})

    direct = (1, 2) if grid else tuple(range(1, n))
    relays = [(1, q) for q in range(CHUNKS // 2)] + [(2, q) for q in range(CHUNKS // 2, CHUNKS)]
    place = jnp.int32(-1)
    order = []
    for s in range(CAP):
        place = following[jnp.minimum(place + 1, blocks)]
        order.append(place)
    halves = (list(range(CHUNKS // 2)), list(range(CHUNKS // 2, CHUNKS)))
    for low, high in zip(*halves):
        for q in (low, high):
            for s in range(q * per, (q + 1) * per):
                gath[0][s] = dressed[order[s]]
        if grid:
            own_copy(1, low).start()
            own_copy(2, high).start()
    if grid:
        for low, high in zip(*halves):
            own_copy(1, high).start()
            own_copy(2, low).start()
    else:
        for k in direct:
            for q in range(CHUNKS):
                own_copy(k, q).start()

    def partner_copy(j, k):
        return remote(give.at[k], take.at[k], p_send.at[k], p_recv.at[k], {"ka": partner})

    def form(k):
        j = src[k]

        def rows(e, count):
            for b in range(col_blocks):
                live = mask[j, e, b]
                block = gath[k][jnp.minimum(count, CAP - 1)]
                dense[pl.ds(pl.multiple_of(e * TILE, TILE), TILE), b * TILE:(b + 1) * TILE] = jnp.where(
                    live != 0, block, jnp.zeros_like(block))
                count = count + live
            return count

        lax.fori_loop(0, row_blocks, rows, jnp.int32(0))
        give[k] = jnp.dot(lam_v[partner, j], dense[...], preferred_element_type=jnp.float32).astype(jnp.bfloat16)
        own[k] = jnp.dot(lam_v[c, j], dense[...], preferred_element_type=jnp.float32)
        partner_copy(j, k).start()

    def out_copy(k):
        return pltpu.make_async_copy(res.at[k], out.at[0, src[k]], o_sem.at[k])

    def finish(k):
        partner_copy(src[k], k).wait_recv()
        res[k] = (own[k] + take[k].astype(jnp.float32)).astype(jnp.bfloat16)
        out_copy(k).start()

    loads[3].wait()
    form(0)
    if grid:
        for k, q in relays:
            own_copy(k, q).wait_recv()
            relay_copy(k, q).start()
        done = set(relays)
    else:
        done = set()
    for k in range(1, n):
        for q in range(CHUNKS):
            if (k, q) not in done:
                own_copy(k, q).wait_recv()
        form(k)
        finish(k - 1)
    finish(n - 1)

    for k in range(1, n):
        t_copies[k].wait_send()
    for k in direct:
        for q in range(CHUNKS):
            own_copy(k, q).wait_send()
    if grid:
        for k, q in relays:
            relay_copy(k, q).wait_send()
    for k in range(n):
        partner_copy(src[k], k).wait_send()
        out_copy(k).wait()


def body(n, lambda_amps, screened_ints, half_ints, singles, block_mask):
    wide, pairs, rows, half = lambda_amps.shape
    full = screened_ints.shape[2]
    inner, width = singles.shape
    blocks = (half // TILE) * (full // TILE)
    bf16, f32 = jnp.bfloat16, jnp.float32
    dma = pltpu.SemaphoreType.DMA
    anywhere = pl.BlockSpec(memory_space=pl.ANY)
    return pl.pallas_call(
        functools.partial(kernel, n),
        out_shape=jax.ShapeDtypeStruct((1, pairs, rows, full), bf16),
        in_specs=[anywhere] * 4 + [pl.BlockSpec(memory_space=pltpu.SMEM)],
        out_specs=anywhere,
        scratch_shapes=[
            pltpu.VMEM(lambda_amps.shape, bf16),
            pltpu.VMEM((half, full), bf16),
            pltpu.VMEM((half, inner), bf16),
            pltpu.VMEM((blocks, TILE, TILE), bf16),
            pltpu.VMEM((half, full), bf16),
            pltpu.VMEM((n, rows, full), f32),
            pltpu.VMEM((n, rows, full), bf16),
            pltpu.VMEM((n, rows, full), bf16),
            pltpu.VMEM((n, rows, full), bf16),
            pltpu.SMEM((blocks + 1,), jnp.int32),
            dma((4,)), dma((n,)), dma((n,)), dma((n, CHUNKS)), dma((n, CHUNKS)), dma((CHUNKS,)),
            dma((n,)), dma((n,)), dma((n,)),
        ] + [pltpu.VMEM((inner, width), bf16)] * n + [pltpu.VMEM((CAP, TILE, TILE), bf16)] * n,
        compiler_params=pltpu.CompilerParams(
            collective_id=0, has_side_effects=True, vmem_limit_bytes=56 * 1024 * 1024),
    )(lambda_amps, screened_ints, half_ints, singles, block_mask)


def solution(mesh):
    return jax.shard_map(
        functools.partial(body, mesh.shape["vir"]),
        mesh=mesh,
        in_specs=(
            P(None, "occ", "vir", "ka"),
            P(("occ", "vir"), "ka", None),
            P(("occ", "vir"), "ka", None),
            P(None, "vir"),
            P("occ", "ka", None),
        ),
        out_specs=P("ka", "occ", "vir", None),
        check_vma=False,
    )
```

```python
import functools

import jax
import jax.numpy as jnp
from jax import lax
from jax.experimental import pallas as pl
from jax.experimental.pallas import tpu as pltpu
from jax.sharding import PartitionSpec as P

TILE = 128
CAP = 16
SIDES = 2
CHUNKS = 4


def peers_of(v, n, grid):
    if grid:
        y, x = v // 2, v % 2
        ids = [v, y * 2 + (1 - x), (1 - y) * 2 + x, (1 - y) * 2 + (1 - x)]
        return ids, ids
    return [(v + k) % n for k in range(n)], [(v + n - k) % n for k in range(n)]


def kernel(n, lam, x, y, t, mask, out, lam_v, x_v, y_v, dressed, dense, own, give, take, following,
           in_sem, t_send, t_recv, h_send, h_recv, b_send, b_recv, f_send, p_send, p_recv, *bufs):
    t_v, gath = bufs[:n], bufs[n:]
    grid = n == 4
    v, c = lax.axis_index("vir"), lax.axis_index("ka")
    dst, src = peers_of(v, n, grid)
    partner = 1 - c
    half = x_v.shape[0]
    width = t_v[0].shape[1]
    cols = width // TILE
    row_blocks = half // TILE
    col_blocks = x_v.shape[1] // TILE
    blocks = row_blocks * col_blocks
    per = CAP // CHUNKS

    loads = [
        pltpu.make_async_copy(t, t_v[0], in_sem.at[0]),
        pltpu.make_async_copy(y.at[0], y_v, in_sem.at[1]),
        pltpu.make_async_copy(x.at[0], x_v, in_sem.at[2]),
        pltpu.make_async_copy(lam, lam_v, in_sem.at[3]),
    ]
    for load in loads:
        load.start()

    barrier = pltpu.get_barrier_semaphore()
    for k in range(1, n):
        pl.semaphore_signal(barrier, inc=1, device_id={"vir": dst[k]}, device_id_type=pl.DeviceIdType.MESH)
    pl.semaphore_signal(barrier, inc=1, device_id={"ka": partner}, device_id_type=pl.DeviceIdType.MESH)
    loads[0].wait()
    pl.semaphore_wait(barrier, n)

    def remote(source, target, send, recv, where):
        return pltpu.make_async_remote_copy(
            src_ref=source, dst_ref=target, send_sem=send, recv_sem=recv,
            device_id=where, device_id_type=pl.DeviceIdType.MESH)

    share = t_v[0].shape[0] // 2
    part_rows = pl.ds(pl.multiple_of(c * share, share), share)
    t_copies = [None] + [
        remote(t_v[0].at[part_rows], t_v[k].at[part_rows], t_send.at[k], t_recv.at[k], {"vir": dst[k]})
        for k in range(1, n)]
    t_swaps = [None] + [
        remote(t_v[k].at[part_rows], t_v[k].at[part_rows], h_send.at[k], h_recv.at[k], {"ka": partner})
        for k in range(1, n)]
    for copy in reversed(t_copies[1:]):
        copy.start()

    following[blocks] = blocks - 1
    later = jnp.int32(blocks - 1)
    for p in reversed(range(blocks)):
        later = jnp.where(mask[v, p // col_blocks, p % col_blocks] != 0, p, later)
        following[p] = later

    loads[1].wait()
    loads[2].wait()

    def dress(k):
        start = src[k] * width
        term = jnp.dot(y_v[...], t_v[k][...], preferred_element_type=jnp.float32)
        part = (x_v[:, pl.ds(pl.multiple_of(start, TILE), width)].astype(jnp.float32) - term).astype(jnp.bfloat16)
        for e in range(row_blocks):
            for b in range(cols):
                dressed[e * col_blocks + src[k] * cols + b] = part[e * TILE:(e + 1) * TILE, b * TILE:(b + 1) * TILE]

    dress(0)
    for k in range(1, n):
        t_copies[k].wait_recv()
        t_swaps[k].start()
    for k in range(1, n):
        t_swaps[k].wait_recv()
        dress(k)

    def chunk(ref, q):
        return ref.at[pl.ds(q * per, per)]

    def own_copy(k, q):
        return remote(chunk(gath[0], q), chunk(gath[k], q), b_send.at[k, q], b_recv.at[k, q], {"vir": dst[k]})

    def relay_copy(k, q):
        return remote(chunk(gath[k], q), chunk(gath[3], q), f_send.at[q], b_recv.at[3, q], {"vir": dst[3 - k]})

    direct = (1, 2) if grid else tuple(range(1, n))
    relays = [(1, q) for q in range(CHUNKS // 2)] + [(2, q) for q in range(CHUNKS // 2, CHUNKS)]
    place = jnp.int32(-1)
    order = []
    for s in range(CAP):
        place = following[jnp.minimum(place + 1, blocks)]
        order.append(place)
    halves = (list(range(CHUNKS // 2)), list(range(CHUNKS // 2, CHUNKS)))
    for low, high in zip(*halves):
        for q in (low, high):
            for s in range(q * per, (q + 1) * per):
                gath[0][s] = dressed[order[s]]
        if grid:
            own_copy(1, low).start()
            own_copy(2, high).start()
    if grid:
        for low, high in zip(*halves):
            own_copy(1, high).start()
            own_copy(2, low).start()
    else:
        for k in direct:
            for q in range(CHUNKS):
                own_copy(k, q).start()

    side = x_v.shape[1] // SIDES

    def partner_copy(k, h):
        columns = pl.ds(h * side, side)
        return remote(give.at[k, :, columns], take.at[k, :, columns], p_send.at[k, h], p_recv.at[k, h], {"ka": partner})

    def form(k):
        j = src[k]

        def rows(e, count):
            for b in range(col_blocks):
                live = mask[j, e, b]
                block = gath[k][jnp.minimum(count, CAP - 1)]
                dense[pl.ds(pl.multiple_of(e * TILE, TILE), TILE), b * TILE:(b + 1) * TILE] = jnp.where(
                    live != 0, block, jnp.zeros_like(block))
                count = count + live
            return count

        lax.fori_loop(0, row_blocks, rows, jnp.int32(0))
        for h in range(SIDES):
            columns = slice(h * side, (h + 1) * side)
            give[k, :, columns] = jnp.dot(
                lam_v[partner, j], dense[:, columns], preferred_element_type=jnp.float32).astype(jnp.bfloat16)
            partner_copy(k, h).start()
        own[k] = jnp.dot(lam_v[c, j], dense[...], preferred_element_type=jnp.float32)

    def finish(k):
        for h in range(SIDES):
            columns = slice(h * side, (h + 1) * side)
            partner_copy(k, h).wait_recv()
            out[0, src[k], :, columns] = (
                own[k, :, columns] + take[k, :, columns].astype(jnp.float32)).astype(jnp.bfloat16)

    loads[3].wait()
    form(0)
    if grid:
        for k, q in relays:
            own_copy(k, q).wait_recv()
            relay_copy(k, q).start()
        done = set(relays)
    else:
        done = set()
    for k in range(1, n):
        for q in range(CHUNKS):
            if (k, q) not in done:
                own_copy(k, q).wait_recv()
        form(k)
        finish(k - 1)
    finish(n - 1)

    for k in range(1, n):
        t_copies[k].wait_send()
        t_swaps[k].wait_send()
    for k in direct:
        for q in range(CHUNKS):
            own_copy(k, q).wait_send()
    if grid:
        for k, q in relays:
            relay_copy(k, q).wait_send()
    for k in range(n):
        for h in range(SIDES):
            partner_copy(k, h).wait_send()


def body(n, lambda_amps, screened_ints, half_ints, singles, block_mask):
    wide, pairs, rows, half = lambda_amps.shape
    full = screened_ints.shape[2]
    inner, width = singles.shape
    blocks = (half // TILE) * (full // TILE)
    bf16, f32 = jnp.bfloat16, jnp.float32
    dma = pltpu.SemaphoreType.DMA
    anywhere = pl.BlockSpec(memory_space=pl.ANY)
    return pl.pallas_call(
        functools.partial(kernel, n),
        out_shape=pltpu.VMEM((1, pairs, rows, full), bf16),
        in_specs=[anywhere] * 4 + [pl.BlockSpec(memory_space=pltpu.SMEM)],
        out_specs=pl.BlockSpec(memory_space=pltpu.VMEM),
        scratch_shapes=[
            pltpu.VMEM(lambda_amps.shape, bf16),
            pltpu.VMEM((half, full), bf16),
            pltpu.VMEM((half, inner), bf16),
            pltpu.VMEM((blocks, TILE, TILE), bf16),
            pltpu.VMEM((half, full), bf16),
            pltpu.VMEM((n, rows, full), f32),
            pltpu.VMEM((n, rows, full), bf16),
            pltpu.VMEM((n, rows, full), bf16),
            pltpu.SMEM((blocks + 1,), jnp.int32),
            dma((4,)), dma((n,)), dma((n,)), dma((n,)), dma((n,)), dma((n, CHUNKS)), dma((n, CHUNKS)), dma((CHUNKS,)),
            dma((n, SIDES)), dma((n, SIDES)),
        ] + [pltpu.VMEM((inner, width), bf16)] * n + [pltpu.VMEM((CAP, TILE, TILE), bf16)] * n,
        compiler_params=pltpu.CompilerParams(
            collective_id=0, has_side_effects=True, vmem_limit_bytes=56 * 1024 * 1024),
    )(lambda_amps, screened_ints, half_ints, singles, block_mask)


def solution(mesh):
    return jax.shard_map(
        functools.partial(body, mesh.shape["vir"]),
        mesh=mesh,
        in_specs=(
            P(None, "occ", "vir", "ka"),
            P(("occ", "vir"), "ka", None),
            P(("occ", "vir"), "ka", None),
            P(None, "vir"),
            P("occ", "ka", None),
        ),
        out_specs=P("ka", "occ", "vir", None),
        check_vma=False,
    )
```

```python
import functools

import jax
import jax.numpy as jnp
from jax import lax
from jax.experimental import pallas as pl
from jax.experimental.pallas import tpu as pltpu
from jax.sharding import PartitionSpec as P

TILE = 128
CAP = 16
SIDES = 2
CHUNKS = 2


def peers_of(v, n, grid):
    if grid:
        y, x = v // 2, v % 2
        ids = [v, y * 2 + (1 - x), (1 - y) * 2 + x, (1 - y) * 2 + (1 - x)]
        return ids, ids
    return [(v + k) % n for k in range(n)], [(v + n - k) % n for k in range(n)]


def kernel(n, lam, x, y, t, mask, out, lam_v, x_v, y_v, dressed, dense, own, give, take, following,
           in_sem, t_send, t_recv, b_send, b_recv, f_send, p_send, p_recv, *bufs):
    t_v, gath = bufs[:n], bufs[n:]
    grid = n == 4
    v, c = lax.axis_index("vir"), lax.axis_index("ka")
    dst, src = peers_of(v, n, grid)
    partner = 1 - c
    half = x_v.shape[0]
    width = t_v[0].shape[1]
    cols = width // TILE
    row_blocks = half // TILE
    col_blocks = x_v.shape[1] // TILE
    blocks = row_blocks * col_blocks
    per = CAP // CHUNKS

    loads = [
        pltpu.make_async_copy(t, t_v[0], in_sem.at[0]),
        pltpu.make_async_copy(y.at[0], y_v, in_sem.at[1]),
        pltpu.make_async_copy(x.at[0], x_v, in_sem.at[2]),
        pltpu.make_async_copy(lam, lam_v, in_sem.at[3]),
    ]
    for load in loads:
        load.start()

    barrier = pltpu.get_barrier_semaphore()
    for k in range(1, n):
        pl.semaphore_signal(barrier, inc=1, device_id={"vir": dst[k]}, device_id_type=pl.DeviceIdType.MESH)
    pl.semaphore_signal(barrier, inc=1, device_id={"ka": partner}, device_id_type=pl.DeviceIdType.MESH)
    loads[0].wait()
    pl.semaphore_wait(barrier, n)

    def remote(source, target, send, recv, where):
        return pltpu.make_async_remote_copy(
            src_ref=source, dst_ref=target, send_sem=send, recv_sem=recv,
            device_id=where, device_id_type=pl.DeviceIdType.MESH)

    t_copies = [None] + [
        remote(t_v[0], t_v[k], t_send.at[k], t_recv.at[k], {"vir": dst[k]})
        for k in range(1, n)]
    for copy in reversed(t_copies[1:]):
        copy.start()

    following[blocks] = blocks - 1
    later = jnp.int32(blocks - 1)
    for p in reversed(range(blocks)):
        later = jnp.where(mask[v, p // col_blocks, p % col_blocks] != 0, p, later)
        following[p] = later

    loads[1].wait()
    loads[2].wait()

    def dress(k):
        start = src[k] * width
        term = jnp.dot(y_v[...], t_v[k][...], preferred_element_type=jnp.float32)
        part = (x_v[:, pl.ds(pl.multiple_of(start, TILE), width)].astype(jnp.float32) - term).astype(jnp.bfloat16)
        for e in range(row_blocks):
            for b in range(cols):
                dressed[e * col_blocks + src[k] * cols + b] = part[e * TILE:(e + 1) * TILE, b * TILE:(b + 1) * TILE]

    dress(0)
    for k in range(1, n):
        t_copies[k].wait_recv()
    for k in range(1, n):
        dress(k)

    def chunk(ref, q):
        return ref.at[pl.ds(q * per, per)]

    def own_copy(k, q):
        return remote(chunk(gath[0], q), chunk(gath[k], q), b_send.at[k, q], b_recv.at[k, q], {"vir": dst[k]})

    def relay_copy(k, q):
        return remote(chunk(gath[k], q), chunk(gath[3], q), f_send.at[q], b_recv.at[3, q], {"vir": dst[3 - k]})

    direct = (1, 2) if grid else tuple(range(1, n))
    relays = [(1, q) for q in range(CHUNKS // 2)] + [(2, q) for q in range(CHUNKS // 2, CHUNKS)]
    place = jnp.int32(-1)
    order = []
    for s in range(CAP):
        place = following[jnp.minimum(place + 1, blocks)]
        order.append(place)
    halves = (list(range(CHUNKS // 2)), list(range(CHUNKS // 2, CHUNKS)))
    for low, high in zip(*halves):
        for q in (low, high):
            for s in range(q * per, (q + 1) * per):
                gath[0][s] = dressed[order[s]]
        if grid:
            own_copy(1, low).start()
            own_copy(2, high).start()
    if grid:
        for low, high in zip(*halves):
            own_copy(1, high).start()
            own_copy(2, low).start()
    else:
        for k in direct:
            for q in range(CHUNKS):
                own_copy(k, q).start()

    side = x_v.shape[1] // SIDES

    def partner_copy(k, h):
        columns = pl.ds(h * side, side)
        return remote(give.at[k, :, columns], take.at[k, :, columns], p_send.at[k, h], p_recv.at[k, h], {"ka": partner})

    def form(k):
        j = src[k]

        def rows(e, count):
            for b in range(col_blocks):
                live = mask[j, e, b]
                block = gath[k][jnp.minimum(count, CAP - 1)]
                dense[pl.ds(pl.multiple_of(e * TILE, TILE), TILE), b * TILE:(b + 1) * TILE] = jnp.where(
                    live != 0, block, jnp.zeros_like(block))
                count = count + live
            return count

        lax.fori_loop(0, row_blocks, rows, jnp.int32(0))
        for h in range(SIDES):
            columns = slice(h * side, (h + 1) * side)
            give[k, :, columns] = jnp.dot(
                lam_v[partner, j], dense[:, columns], preferred_element_type=jnp.float32).astype(jnp.bfloat16)
            partner_copy(k, h).start()
        own[k] = jnp.dot(lam_v[c, j], dense[...], preferred_element_type=jnp.float32)

    def finish(k):
        for h in range(SIDES):
            columns = slice(h * side, (h + 1) * side)
            partner_copy(k, h).wait_recv()
            out[0, src[k], :, columns] = (
                own[k, :, columns] + take[k, :, columns].astype(jnp.float32)).astype(jnp.bfloat16)

    loads[3].wait()
    form(0)
    if grid:
        for k, q in relays:
            own_copy(k, q).wait_recv()
            relay_copy(k, q).start()
        done = set(relays)
    else:
        done = set()
    for k in range(1, n):
        if k == n - 1:
            finish(k - 1)
        for q in range(CHUNKS):
            if (k, q) not in done:
                own_copy(k, q).wait_recv()
        form(k)
        if k < n - 1:
            finish(k - 1)
    finish(n - 1)

    for k in range(1, n):
        t_copies[k].wait_send()
    for k in direct:
        for q in range(CHUNKS):
            own_copy(k, q).wait_send()
    if grid:
        for k, q in relays:
            relay_copy(k, q).wait_send()
    for k in range(n):
        for h in range(SIDES):
            partner_copy(k, h).wait_send()


def body(n, lambda_amps, screened_ints, half_ints, singles, block_mask):
    wide, pairs, rows, half = lambda_amps.shape
    full = screened_ints.shape[2]
    inner, width = singles.shape
    blocks = (half // TILE) * (full // TILE)
    bf16, f32 = jnp.bfloat16, jnp.float32
    dma = pltpu.SemaphoreType.DMA
    anywhere = pl.BlockSpec(memory_space=pl.ANY)
    return pl.pallas_call(
        functools.partial(kernel, n),
        out_shape=pltpu.VMEM((1, pairs, rows, full), bf16),
        in_specs=[anywhere] * 4 + [pl.BlockSpec(memory_space=pltpu.SMEM)],
        out_specs=pl.BlockSpec(memory_space=pltpu.VMEM),
        scratch_shapes=[
            pltpu.VMEM(lambda_amps.shape, bf16),
            pltpu.VMEM((half, full), bf16),
            pltpu.VMEM((half, inner), bf16),
            pltpu.VMEM((blocks, TILE, TILE), bf16),
            pltpu.VMEM((half, full), bf16),
            pltpu.VMEM((n, rows, full), f32),
            pltpu.VMEM((n, rows, full), bf16),
            pltpu.VMEM((n, rows, full), bf16),
            pltpu.SMEM((blocks + 1,), jnp.int32),
            dma((4,)), dma((n,)), dma((n,)), dma((n, CHUNKS)), dma((n, CHUNKS)), dma((CHUNKS,)),
            dma((n, SIDES)), dma((n, SIDES)),
        ] + [pltpu.VMEM((inner, width), bf16)] * n + [pltpu.VMEM((CAP, TILE, TILE), bf16)] * n,
        compiler_params=pltpu.CompilerParams(
            collective_id=0, has_side_effects=True, vmem_limit_bytes=56 * 1024 * 1024),
    )(lambda_amps, screened_ints, half_ints, singles, block_mask)


def solution(mesh):
    return jax.shard_map(
        functools.partial(body, mesh.shape["vir"]),
        mesh=mesh,
        in_specs=(
            P(None, "occ", "vir", "ka"),
            P(("occ", "vir"), "ka", None),
            P(("occ", "vir"), "ka", None),
            P(None, "vir"),
            P("occ", "ka", None),
        ),
        out_specs=P("ka", "occ", "vir", None),
        check_vma=False,
    )
```
